32 devices in a mesh: dp: 2 (over x), vocab: 16 (over z, y, core).
Axes of the slice: x: 2, y: 2, z: 4, core: 2. Of those that a mesh axis runs over, the one named last changes fastest.
Arguments:
- hidden: bfloat16 [96, 8192], P('dp', 'vocab'), may hold values from -90 to 90
- weight: bfloat16 [8192, 38016], P('dp', 'vocab'), may hold values from -0.1875 to 0.1875
- targets: int32 [96], P('dp'), may hold values from 0 to 38015
- pad_mask: int32 [96], P('dp'), may hold values from 0 to 1
Outputs:
- token_nll: float32 [96], P('dp')
- nll_total: float32 [], replicated
The draws below stay inside these ranges and needn't reach their ends.
All inputs are finite; a program needn't handle non-finite values.
Results may differ from the reference program's by a relative error of at most 0.0003.
Values may be sent and summed in bfloat16 or wider, within the bound.
A program may use at most 64 MiB of HBM per device.

```python
import math
import jax
import jax.numpy as jnp
import numpy as np

D = 8192
TOKENS = 96
VOCAB = 38016
N_DP = 2


def draw_hidden(key, part):
    base = jax.random.truncated_normal(key, -6.0, 6.0, (TOKENS, D), jnp.float32)
    return base.astype(jnp.bfloat16)


def draw_pad_mask(key, part):
    positions = jnp.arange(TOKENS)
    level = 25 + 70 * positions // TOKENS
    return (jax.random.randint(key, (TOKENS,), 0, 100) < level).astype(jnp.int32)


def set_ends(values, own_key, least, largest):
    shape = values.shape
    place = [jax.random.randint(jax.random.fold_in(own_key, axis), (), 0, shape[axis]) for axis in range(len(shape))]
    values = values.at[tuple(place)].set(least)
    longest = shape.index(max(shape))
    place[longest] = (place[longest] + 1) % shape[longest]
    return values.at[tuple(place)].set(largest)


def level_of(rng, dims, shards, low, high):
    factor_of, own = 1.0, jax.random.fold_in(rng, 6)
    for dim, shards_of in shards:
        heights = jnp.exp(jax.random.uniform(jax.random.fold_in(own, dim), (shards_of,), jnp.float32, low / len(shards), high / len(shards)))
        factor_of = factor_of * jnp.repeat(heights, dims[dim] // shards_of).reshape([-1 if axis == dim else 1 for axis in range(len(dims))])
    return factor_of


def rank_bounds(amount, skew):
    portions = [(1 << 20) // math.isqrt(rank ** skew) + 1 for rank in range(1, amount + 1)]
    deviation = 1 + sum(portions) // (1 << 30)
    return np.cumsum(np.array([max(1, weight // deviation) for weight in portions]))


def ranked_ids(stream_key, extent, number_of, skew):
    grid = rank_bounds(number_of, skew)
    ticket = jax.random.randint(jax.random.fold_in(stream_key, 1), extent, 0, int(grid[number_of - 1]))
    grade = jnp.searchsorted(jnp.asarray(grid, jnp.int32), ticket, side="right")
    return jax.random.permutation(jax.random.fold_in(stream_key, 2), number_of)[grade].astype(jnp.int32)


def normal_values(own_key, dims, spread, limit, pieces=(), held_as=jnp.bfloat16):
    entries = jax.random.normal(own_key, dims, jnp.float32) * spread
    if len(pieces) > 0:
        entries = level_of(own_key, dims, pieces, -0.22, 0.18) * entries
    return jnp.clip(entries, min=-limit, max=limit).astype(held_as)


def setup_inputs(seed: int = 0) -> dict:
    keys = jax.random.split(jax.random.key(seed), 5)
    hidden = draw_hidden(jax.random.fold_in(keys[4], 71), 0)
    weight = normal_values(keys[1], (D, VOCAB), (D // 9) ** -0.5, 0.1875, ((0, 2), (1, 16)))
    targets = set_ends(ranked_ids(keys[2], (TOKENS,), VOCAB, 2), jax.random.fold_in(keys[2], 3), 0, VOCAB - 1).astype(jnp.int32)
    pad_mask = draw_pad_mask(jax.random.fold_in(keys[4], 71), 0)
    return {"hidden": hidden, "weight": weight, "targets": targets, "pad_mask": pad_mask}


def reference(hidden, weight, targets, pad_mask):
    slab = D // N_DP
    logits = jnp.zeros((TOKENS, VOCAB), jnp.float32)
    for block in range(N_DP):
        partial_value = jnp.dot(hidden[:, block * slab:(block + 1) * slab], weight[block * slab:(block + 1) * slab, :], preferred_element_type=jnp.float32)
        logits = logits + partial_value
    row_max = jnp.max(logits, axis=1)
    exp_sum = jnp.sum(jnp.exp(logits - row_max[:, None]), axis=1)
    picked = jnp.take_along_axis(logits, targets[:, None].astype(jnp.int32), axis=1)[:, 0]
    token_nll = pad_mask.astype(jnp.float32) * (row_max + jnp.log(exp_sum) - picked)
    return token_nll, jnp.sum(token_nll)
```

```python
import functools

import jax
import jax.numpy as jnp
from jax import lax
from jax.experimental import pallas as pl
from jax.experimental.pallas import tpu as pltpu
from jax.sharding import PartitionSpec as P

N_CHUNKS = 3
LANES = 128
MESH = pl.DeviceIdType.MESH


def chunk_bounds(cols):
    width = max(LANES, cols // N_CHUNKS // LANES * LANES)
    starts = [i * width for i in range(N_CHUNKS)]
    return [(s, (cols - s) if i == N_CHUNKS - 1 else width) for i, s in enumerate(starts)]


def padded(width):
    return -(-width // LANES) * LANES


def kernel(n_dp, n_v, n_r, n_c, hid, w_hbm, tgt, msk, nll_out, tot_out,
           toks, w, acc, stat_in, stat_out, square,
           own_sem, w_sem, recv, line_send, plane_send, part_send,
           rs_send, rs_recv, st_send, st_recv, *codes):
    send_q, recv_q = codes[:N_CHUNKS], codes[N_CHUNKS:]
    t_loc, depth = hid.shape
    cols = w_hbm.shape[1]
    group = n_v // n_dp
    r_group = n_r // n_dp
    half = group // 2
    d = lax.axis_index("dp")
    v = lax.axis_index("vocab")
    k = lax.rem(v, 2)
    c = lax.rem(v // 2, n_c)
    r = v // (2 * n_c)

    def vid(rr, cc, kk):
        return (rr * n_c + cc) * 2 + kk

    def chunk_vid(i):
        k_off, idx = i // half, lax.rem(i, half)
        rr = d * r_group + lax.rem(idx // n_c + r, r_group)
        cc = lax.rem(idx + c, n_c)
        return vid(rr, cc, lax.rem(k + k_off, 2))

    def weight_copy(i):
        rows = pl.ds(pl.multiple_of((chunk_vid(i) - d * group) * depth, depth), depth)
        return pltpu.make_async_copy(w_hbm.at[rows, :], w.at[rows, :], w_sem.at[i])

    own = pltpu.make_async_copy(hid, toks.at[v, d], own_sem)
    own.start()

    def start_weight(i, carry):
        weight_copy(i).start()
        return carry

    lax.fori_loop(0, group, start_weight, 0)

    barrier = pltpu.get_barrier_semaphore()

    def greet(dd, vv):
        pl.semaphore_signal(barrier, inc=1, device_id={"dp": dd, "vocab": vv}, device_id_type=MESH)

    for o in range(1, n_r):
        greet(d, vid(lax.rem(r + o, n_r), c, k))
    for do in range(n_dp):
        for co in range(n_c):
            if do or co:
                greet(lax.rem(d + do, n_dp), vid(r, lax.rem(c + co, n_c), k))
    greet(d, vid(r, c, 1 - k))
    pl.semaphore_wait(barrier, n_r - 1 + n_dp * n_c - 1 + 1)

    def piece_copy(src, vv, dd, send_sem, to_d, to_v):
        return pltpu.make_async_remote_copy(
            src_ref=src, dst_ref=toks.at[vv, dd], send_sem=send_sem, recv_sem=recv.at[vv, dd],
            device_id={"dp": to_d, "vocab": to_v}, device_id_type=MESH)

    def arrived(vv, dd):
        pltpu.make_async_copy(hid, toks.at[vv, dd], recv.at[vv, dd]).wait()

    partner = vid(r, c, 1 - k)

    def line_copy(o):
        return piece_copy(hid, v, d, line_send.at[o], d, vid(lax.rem(r + o, n_r), c, k))

    def plane_copy(o, co):
        rr = lax.rem(r + o, n_r)
        mine = vid(rr, c, k)
        src = hid if o == 0 else toks.at[mine, d]
        return piece_copy(src, mine, d, plane_send.at[o, co], rr // r_group,
                          vid(r, lax.rem(c + co, n_c), k))

    def own_line_part(o):
        rr = lax.rem(r + o, n_r)
        mine = vid(rr, c, k)
        src = hid if o == 0 else toks.at[mine, d]
        return piece_copy(src, mine, d, part_send.at[mine // 2, d], d, partner)

    def spread(o, act):
        rr = lax.rem(r + o, n_r)
        home = rr // r_group == d
        for co in range(1, n_c):
            act(plane_copy(o, co))

        @pl.when(jnp.logical_not(home))
        def _():
            act(plane_copy(o, 0))

        @pl.when(home)
        def _():
            act(own_line_part(o))

    start = lambda copy: copy.start()
    sent = lambda copy: copy.wait_send()

    for o in range(1, n_r):
        line_copy(o).start()
    spread(0, start)
    for o in range(1, n_r):
        arrived(vid(lax.rem(r + o, n_r), c, k), d)
        spread(o, start)

    def plane_pieces(act):
        for ro in range(r_group):
            rr = d * r_group + lax.rem(r + ro, r_group)
            for do in range(n_dp):
                for co in range(n_c):
                    if do or co:
                        act(vid(rr, lax.rem(c + co, n_c), k), lax.rem(d + do, n_dp))

    def part_copy(vv, dd):
        return piece_copy(toks.at[vv, dd], vv, dd, part_send.at[vv // 2, dd], d, partner)

    def relay(vv, dd):
        arrived(vv, dd)
        part_copy(vv, dd).start()

    plane_pieces(relay)
    own.wait()

    def tokens_of(vv):
        return toks[vv].reshape(n_dp * t_loc, depth)

    def rows_of(vv):
        return pl.ds(pl.multiple_of((vv - d * group) * depth, depth), depth)

    def first_half(i, carry):
        vv = chunk_vid(i)
        weight_copy(i).wait()
        part = jnp.dot(tokens_of(vv), w[rows_of(vv), :], preferred_element_type=jnp.float32)
        part = part.reshape(n_dp, t_loc, cols)

        @pl.when(i == 0)
        def _():
            acc[...] = part

        @pl.when(i > 0)
        def _():
            acc[...] += part

        return carry

    lax.fori_loop(0, half, first_half, 0)

    def second_ready(i, carry):
        vv = chunk_vid(i)
        weight_copy(i).wait()
        for dd in range(n_dp):
            arrived(vv, dd)
        return carry

    lax.fori_loop(half, group, second_ready, 0)

    bounds = chunk_bounds(cols)

    def rs_copy(ch, o):
        peer = lax.rem(d + o, n_dp)
        return pltpu.make_async_remote_copy(
            src_ref=send_q[ch].at[peer], dst_ref=recv_q[ch].at[d],
            send_sem=rs_send.at[ch, o], recv_sem=rs_recv.at[ch, n_dp - o],
            device_id={"dp": peer}, device_id_type=MESH)

    for ch, (lo, width) in enumerate(bounds):
        cut = slice(lo, lo + width)
        total = acc[:, :, cut].reshape(n_dp * t_loc, width)
        for i in range(half, group):
            vv = chunk_vid(i)
            total += jnp.dot(tokens_of(vv), w[rows_of(vv), cut], preferred_element_type=jnp.float32)
        acc[:, :, cut] = total.reshape(n_dp, t_loc, width)
        for o in range(1, n_dp):
            peer = lax.rem(d + o, n_dp)
            mine = acc[peer, :, cut]
            top = jnp.maximum(jnp.max(jnp.abs(mine), axis=1, keepdims=True), 1e-30)
            expo = jnp.floor(jnp.log2(top)).astype(jnp.int32) + 2
            unit = jnp.exp2((15 - expo).astype(jnp.float32))
            code = jnp.round(mine * unit).astype(jnp.int32)
            send_q[ch][peer, :, :width] = code.astype(jnp.int16)
            wide = jnp.broadcast_to(expo, (t_loc, LANES))
            send_q[ch][peer, :, padded(width):] = wide.astype(jnp.int16)
            rs_copy(ch, o).start()

    maxes, sums, picks = [], [], []
    for ch, (lo, width) in enumerate(bounds):
        cut = slice(lo, lo + width)
        logits = acc[d, :, cut]
        for o in range(1, n_dp):
            src = lax.rem(d + n_dp - o, n_dp)
            pltpu.make_async_copy(send_q[ch].at[d], recv_q[ch].at[src], rs_recv.at[ch, n_dp - o]).wait()
            code = recv_q[ch][src, :, :width].astype(jnp.int32).astype(jnp.float32)
            expo = recv_q[ch][src, :, padded(width):].astype(jnp.int32)[:, :1]
            logits = logits + code * jnp.exp2((expo - 15).astype(jnp.float32))
        m = jnp.max(logits, axis=1, keepdims=True)
        ids = lax.broadcasted_iota(jnp.int32, (t_loc, width), 1) + (v * cols + lo)
        maxes.append(m)
        sums.append(jnp.sum(jnp.exp(logits - m), axis=1, keepdims=True))
        picks.append(jnp.sum(jnp.where(ids == tgt[...], logits, 0.0), axis=1, keepdims=True))
    top = functools.reduce(jnp.maximum, maxes)
    exp_sum = sum(s * jnp.exp(m - top) for s, m in zip(sums, maxes))
    pick = sum(picks)

    lane = lax.broadcasted_iota(jnp.int32, (t_loc, LANES), 1)
    mask = msk[...].astype(jnp.float32)
    packed = jnp.where(lane == 0, top, jnp.where(lane == 1, exp_sum, jnp.where(
        lane == 2, pick, jnp.where(lane == 3, mask, 0.0))))
    square[...] = jnp.zeros_like(square)
    square[:t_loc, :] = packed
    stat_out[...] = square[...].T[:8, :]
    stat_in[d, v] = stat_out[...]

    n_all = n_dp * n_v
    me = d * n_v + v

    def stat_copy(o):
        to = lax.rem(me + o, n_all)
        return pltpu.make_async_remote_copy(
            src_ref=stat_out, dst_ref=stat_in.at[d, v], send_sem=st_send.at[o],
            recv_sem=st_recv.at[n_all - o],
            device_id={"dp": to // n_v, "vocab": lax.rem(to, n_v)}, device_id_type=MESH)

    def start_stat(o, carry):
        stat_copy(o).start()
        return carry

    lax.fori_loop(1, n_all, start_stat, 0)

    def wait_stat(o, carry):
        src = lax.rem(me + o, n_all)
        pltpu.make_async_copy(
            stat_out, stat_in.at[src // n_v, lax.rem(src, n_v)], st_recv.at[o]).wait()
        return carry

    lax.fori_loop(1, n_all, wait_stat, 0)

    lane1 = lax.broadcasted_iota(jnp.int32, (1, LANES), 1)
    total = jnp.zeros((1, LANES), jnp.float32)
    for dd in range(n_dp):
        row = stat_in[dd]
        all_max = row[:, 0, :]
        m = jnp.max(all_max, axis=0, keepdims=True)
        s = jnp.sum(row[:, 1, :] * jnp.exp(all_max - m), axis=0, keepdims=True)
        p = jnp.sum(row[:, 2, :], axis=0, keepdims=True)
        nll = jnp.where(lane1 < t_loc, row[0, 3:4, :] * (m + jnp.log(s) - p), 0.0)
        total += nll

        @pl.when(d == dd)
        def _():
            nll_out[...] = nll[:, :t_loc]

    tot_out[...] = jnp.sum(total, axis=1, keepdims=True)

    for o in range(1, n_r):
        line_copy(o).wait_send()
    for o in range(n_r):
        spread(o, sent)
    plane_pieces(lambda vv, dd: part_copy(vv, dd).wait_send())
    for ch in range(N_CHUNKS):
        for o in range(1, n_dp):
            rs_copy(ch, o).wait_send()

    def end_stat(o, carry):
        stat_copy(o).wait_send()
        return carry

    lax.fori_loop(1, n_all, end_stat, 0)


def columns_of(n_chips):
    side = 1
    while side * side * 4 <= n_chips:
        side *= 2
    return side


def per_device(n_dp, n_v, hidden, weight, targets, pad_mask):
    t_loc, depth = hidden.shape
    rows, cols = weight.shape
    n_c = columns_of(n_v // 2)
    n_r = n_v // 2 // n_c
    widths = [padded(width) + LANES for _, width in chunk_bounds(cols)]
    dma = pltpu.SemaphoreType.DMA
    any_spec = pl.BlockSpec(memory_space=pl.ANY)
    vmem = pl.BlockSpec(memory_space=pltpu.VMEM)
    codes = [pltpu.VMEM((n_dp, t_loc, width), jnp.int16) for width in widths]
    nll, total = pl.pallas_call(
        functools.partial(kernel, n_dp, n_v, n_r, n_c),
        out_shape=(jax.ShapeDtypeStruct((1, t_loc), jnp.float32),
                   jax.ShapeDtypeStruct((1, 1), jnp.float32)),
        in_specs=[any_spec, any_spec, vmem, vmem],
        out_specs=(vmem, vmem),
        scratch_shapes=[
            pltpu.VMEM((n_v, n_dp, t_loc, depth), jnp.bfloat16),
            pltpu.VMEM((rows, cols), jnp.bfloat16),
            pltpu.VMEM((n_dp, t_loc, cols), jnp.float32),
            pltpu.VMEM((n_dp, n_v, 8, LANES), jnp.float32),
            pltpu.VMEM((8, LANES), jnp.float32),
            pltpu.VMEM((LANES, LANES), jnp.float32),
            dma, dma((n_v // n_dp,)), dma((n_v, n_dp)),
            dma((n_r,)), dma((n_r, n_c)), dma((n_v // 2, n_dp)),
            dma((N_CHUNKS, n_dp)), dma((N_CHUNKS, n_dp)),
            dma((n_dp * n_v,)), dma((n_dp * n_v,)),
            *codes, *codes,
        ],
        compiler_params=pltpu.CompilerParams(
            collective_id=0, has_side_effects=True, vmem_limit_bytes=60 * 1024 * 1024),
    )(hidden, weight, targets[:, None], pad_mask[:, None])
    return nll.reshape(t_loc), total.reshape(())


def solution(mesh):
    placed = (P("dp", "vocab"), P("dp", "vocab"), P("dp"), P("dp"))
    body = functools.partial(per_device, mesh.shape["dp"], mesh.shape["vocab"])
    return jax.shard_map(
        body, mesh=mesh, in_specs=placed, out_specs=(P("dp"), P()), check_vma=False
    )
```

```python
import functools

import jax
import jax.numpy as jnp
from jax import lax
from jax.experimental import pallas as pl
from jax.experimental.pallas import tpu as pltpu
from jax.sharding import PartitionSpec as P

N_CHUNKS = 3
LANES = 128
MESH = pl.DeviceIdType.MESH


def chunk_bounds(cols):
    width = max(LANES, cols // N_CHUNKS // LANES * LANES)
    starts = [i * width for i in range(N_CHUNKS)]
    return [(s, (cols - s) if i == N_CHUNKS - 1 else width) for i, s in enumerate(starts)]


def padded(width):
    return -(-width // LANES) * LANES


def product(tokens, heads):
    return lax.dot_general(tokens, heads, (((1,), (1,)), ((), ())), preferred_element_type=jnp.float32)


def kernel(n_dp, n_v, n_r, n_c, hid, w_hbm, tgt, msk, nll_out, tot_out,
           toks, w, acc, stat_in, stat_out, square,
           own_sem, w_sem, recv, line_send, plane_send, part_send,
           rs_send, rs_recv, st_send, st_recv, *codes):
    send_q, recv_q = codes[:N_CHUNKS], codes[N_CHUNKS:]
    t_loc, depth = hid.shape
    cols = w_hbm.shape[0]
    group = n_v // n_dp
    r_group = n_r // n_dp
    half = group // 2
    d = lax.axis_index("dp")
    v = lax.axis_index("vocab")
    k = lax.rem(v, 2)
    c = lax.rem(v // 2, n_c)
    r = v // (2 * n_c)

    def vid(rr, cc, kk):
        return (rr * n_c + cc) * 2 + kk

    def chunk_vid(i):
        k_off, idx = i // half, lax.rem(i, half)
        rr = d * r_group + lax.rem(idx // n_c + r, r_group)
        cc = lax.rem(idx + c, n_c)
        return vid(rr, cc, lax.rem(k + k_off, 2))

    def weight_copy(i):
        rows = pl.ds(pl.multiple_of((chunk_vid(i) - d * group) * depth, depth), depth)
        return pltpu.make_async_copy(w_hbm.at[:, rows], w.at[:, rows], w_sem.at[i])

    own = pltpu.make_async_copy(hid, toks.at[v, d], own_sem)
    own.start()

    def start_weight(i, carry):
        weight_copy(i).start()
        return carry

    lax.fori_loop(0, group, start_weight, 0)

    barrier = pltpu.get_barrier_semaphore()

    def greet(dd, vv):
        pl.semaphore_signal(barrier, inc=1, device_id={"dp": dd, "vocab": vv}, device_id_type=MESH)

    for o in range(1, n_r):
        greet(d, vid(lax.rem(r + o, n_r), c, k))
    for do in range(n_dp):
        for co in range(n_c):
            if do or co:
                greet(lax.rem(d + do, n_dp), vid(r, lax.rem(c + co, n_c), k))
    greet(d, vid(r, c, 1 - k))
    pl.semaphore_wait(barrier, n_r - 1 + n_dp * n_c - 1 + 1)

    def piece_copy(src, vv, dd, send_sem, to_d, to_v):
        return pltpu.make_async_remote_copy(
            src_ref=src, dst_ref=toks.at[vv, dd], send_sem=send_sem, recv_sem=recv.at[vv, dd],
            device_id={"dp": to_d, "vocab": to_v}, device_id_type=MESH)

    def arrived(vv, dd):
        pltpu.make_async_copy(hid, toks.at[vv, dd], recv.at[vv, dd]).wait()

    partner = vid(r, c, 1 - k)

    def line_copy(o):
        return piece_copy(hid, v, d, line_send.at[o], d, vid(lax.rem(r + o, n_r), c, k))

    def plane_copy(o, co):
        rr = lax.rem(r + o, n_r)
        mine = vid(rr, c, k)
        src = hid if o == 0 else toks.at[mine, d]
        return piece_copy(src, mine, d, plane_send.at[o, co], rr // r_group,
                          vid(r, lax.rem(c + co, n_c), k))

    def own_line_part(o):
        rr = lax.rem(r + o, n_r)
        mine = vid(rr, c, k)
        src = hid if o == 0 else toks.at[mine, d]
        return piece_copy(src, mine, d, part_send.at[mine // 2, d], d, partner)

    def spread(o, act):
        rr = lax.rem(r + o, n_r)
        home = rr // r_group == d
        for co in range(1, n_c):
            act(plane_copy(o, co))

        @pl.when(jnp.logical_not(home))
        def _():
            act(plane_copy(o, 0))

        @pl.when(home)
        def _():
            act(own_line_part(o))

    start = lambda copy: copy.start()
    sent = lambda copy: copy.wait_send()

    for o in range(1, n_r):
        line_copy(o).start()
    spread(0, start)
    for o in range(1, n_r):
        arrived(vid(lax.rem(r + o, n_r), c, k), d)
        spread(o, start)

    def plane_pieces(act):
        for ro in range(r_group):
            rr = d * r_group + lax.rem(r + ro, r_group)
            for do in range(n_dp):
                for co in range(n_c):
                    if do or co:
                        act(vid(rr, lax.rem(c + co, n_c), k), lax.rem(d + do, n_dp))

    def part_copy(vv, dd):
        return piece_copy(toks.at[vv, dd], vv, dd, part_send.at[vv // 2, dd], d, partner)

    def relay(vv, dd):
        arrived(vv, dd)
        part_copy(vv, dd).start()

    plane_pieces(relay)
    own.wait()

    def tokens_of(vv):
        return toks[vv].reshape(n_dp * t_loc, depth)

    def rows_of(vv):
        return pl.ds(pl.multiple_of((vv - d * group) * depth, depth), depth)

    def first_half(i, carry):
        vv = chunk_vid(i)
        weight_copy(i).wait()
        part = product(tokens_of(vv), w[:, rows_of(vv)])
        part = part.reshape(n_dp, t_loc, cols)

        @pl.when(i == 0)
        def _():
            acc[...] = part

        @pl.when(i > 0)
        def _():
            acc[...] += part

        return carry

    lax.fori_loop(0, half, first_half, 0)

    def second_ready(i, carry):
        vv = chunk_vid(i)
        weight_copy(i).wait()
        for dd in range(n_dp):
            arrived(vv, dd)
        return carry

    lax.fori_loop(half, group, second_ready, 0)

    bounds = chunk_bounds(cols)

    def rs_copy(ch, o):
        peer = lax.rem(d + o, n_dp)
        return pltpu.make_async_remote_copy(
            src_ref=send_q[ch].at[peer], dst_ref=recv_q[ch].at[d],
            send_sem=rs_send.at[ch, o], recv_sem=rs_recv.at[ch, n_dp - o],
            device_id={"dp": peer}, device_id_type=MESH)

    for ch, (lo, width) in enumerate(bounds):
        cut = slice(lo, lo + width)
        total = acc[:, :, cut].reshape(n_dp * t_loc, width)
        for i in range(half, group):
            vv = chunk_vid(i)
            total += product(tokens_of(vv), w[cut, rows_of(vv)])
        acc[:, :, cut] = total.reshape(n_dp, t_loc, width)
        for o in range(1, n_dp):
            peer = lax.rem(d + o, n_dp)
            mine = acc[peer, :, cut]
            top = jnp.maximum(jnp.max(jnp.abs(mine), axis=1, keepdims=True), 1e-30)
            expo = jnp.floor(jnp.log2(top)).astype(jnp.int32) + 2
            unit = jnp.exp2((15 - expo).astype(jnp.float32))
            code = jnp.round(mine * unit).astype(jnp.int32)
            send_q[ch][peer, :, :width] = code.astype(jnp.int16)
            wide = jnp.broadcast_to(expo, (t_loc, LANES))
            send_q[ch][peer, :, padded(width):] = wide.astype(jnp.int16)
            rs_copy(ch, o).start()

    square[...] = jnp.zeros_like(square)
    square[:, :t_loc] = jnp.broadcast_to(tgt[...].astype(jnp.float32), (LANES, t_loc))
    wanted = square[...].T[:t_loc, :1].astype(jnp.int32)
    maxes, sums, picks = [], [], []
    for ch, (lo, width) in enumerate(bounds):
        cut = slice(lo, lo + width)
        logits = acc[d, :, cut]
        for o in range(1, n_dp):
            src = lax.rem(d + n_dp - o, n_dp)
            pltpu.make_async_copy(send_q[ch].at[d], recv_q[ch].at[src], rs_recv.at[ch, n_dp - o]).wait()
            code = recv_q[ch][src, :, :width].astype(jnp.int32).astype(jnp.float32)
            expo = recv_q[ch][src, :, padded(width):].astype(jnp.int32)[:, :1]
            logits = logits + code * jnp.exp2((expo - 15).astype(jnp.float32))
        m = jnp.max(logits, axis=1, keepdims=True)
        ids = lax.broadcasted_iota(jnp.int32, (t_loc, width), 1) + (v * cols + lo)
        maxes.append(m)
        sums.append(jnp.sum(jnp.exp(logits - m), axis=1, keepdims=True))
        picks.append(jnp.sum(jnp.where(ids == wanted, logits, 0.0), axis=1, keepdims=True))
    top = functools.reduce(jnp.maximum, maxes)
    exp_sum = sum(s * jnp.exp(m - top) for s, m in zip(sums, maxes))
    pick = sum(picks)

    lane = lax.broadcasted_iota(jnp.int32, (t_loc, LANES), 1)
    packed = jnp.where(lane == 0, top, jnp.where(lane == 1, exp_sum, jnp.where(lane == 2, pick, 0.0)))
    square[...] = jnp.zeros_like(square)
    square[:t_loc, :] = packed
    stat_out[...] = square[...].T[:8, :]
    stat_out[3:4, :t_loc] = msk[...].astype(jnp.float32)
    stat_in[d, v] = stat_out[...]

    n_all = n_dp * n_v
    me = d * n_v + v

    def stat_copy(o):
        to = lax.rem(me + o, n_all)
        return pltpu.make_async_remote_copy(
            src_ref=stat_out, dst_ref=stat_in.at[d, v], send_sem=st_send.at[o],
            recv_sem=st_recv.at[n_all - o],
            device_id={"dp": to // n_v, "vocab": lax.rem(to, n_v)}, device_id_type=MESH)

    def start_stat(o, carry):
        stat_copy(o).start()
        return carry

    lax.fori_loop(1, n_all, start_stat, 0)

    def wait_stat(o, carry):
        src = lax.rem(me + o, n_all)
        pltpu.make_async_copy(
            stat_out, stat_in.at[src // n_v, lax.rem(src, n_v)], st_recv.at[o]).wait()
        return carry

    lax.fori_loop(1, n_all, wait_stat, 0)

    lane1 = lax.broadcasted_iota(jnp.int32, (1, LANES), 1)
    total = jnp.zeros((1, LANES), jnp.float32)
    for dd in range(n_dp):
        row = stat_in[dd]
        all_max = row[:, 0, :]
        m = jnp.max(all_max, axis=0, keepdims=True)
        s = jnp.sum(row[:, 1, :] * jnp.exp(all_max - m), axis=0, keepdims=True)
        p = jnp.sum(row[:, 2, :], axis=0, keepdims=True)
        nll = jnp.where(lane1 < t_loc, row[0, 3:4, :] * (m + jnp.log(s) - p), 0.0)
        total += nll

        @pl.when(d == dd)
        def _():
            nll_out[...] = nll[:, :t_loc]

    tot_out[...] = jnp.sum(total, axis=1, keepdims=True)

    for o in range(1, n_r):
        line_copy(o).wait_send()
    for o in range(n_r):
        spread(o, sent)
    plane_pieces(lambda vv, dd: part_copy(vv, dd).wait_send())
    for ch in range(N_CHUNKS):
        for o in range(1, n_dp):
            rs_copy(ch, o).wait_send()

    def end_stat(o, carry):
        stat_copy(o).wait_send()
        return carry

    lax.fori_loop(1, n_all, end_stat, 0)


def columns_of(n_chips):
    side = 1
    while side * side * 4 <= n_chips:
        side *= 2
    return side


def per_device(n_dp, n_v, hidden, weight, targets, pad_mask):
    t_loc, depth = hidden.shape
    rows, cols = weight.shape
    n_c = columns_of(n_v // 2)
    n_r = n_v // 2 // n_c
    widths = [padded(width) + LANES for _, width in chunk_bounds(cols)]
    dma = pltpu.SemaphoreType.DMA
    any_spec = pl.BlockSpec(memory_space=pl.ANY)
    vmem = pl.BlockSpec(memory_space=pltpu.VMEM)
    codes = [pltpu.VMEM((n_dp, t_loc, width), jnp.int16) for width in widths]
    nll, total = pl.pallas_call(
        functools.partial(kernel, n_dp, n_v, n_r, n_c),
        out_shape=(jax.ShapeDtypeStruct((1, t_loc), jnp.float32),
                   jax.ShapeDtypeStruct((1, 1), jnp.float32)),
        in_specs=[any_spec, any_spec, vmem, vmem],
        out_specs=(vmem, vmem),
        scratch_shapes=[
            pltpu.VMEM((n_v, n_dp, t_loc, depth), jnp.bfloat16),
            pltpu.VMEM((cols, rows), jnp.bfloat16),
            pltpu.VMEM((n_dp, t_loc, cols), jnp.float32),
            pltpu.VMEM((n_dp, n_v, 8, LANES), jnp.float32),
            pltpu.VMEM((8, LANES), jnp.float32),
            pltpu.VMEM((LANES, LANES), jnp.float32),
            dma, dma((n_v // n_dp,)), dma((n_v, n_dp)),
            dma((n_r,)), dma((n_r, n_c)), dma((n_v // 2, n_dp)),
            dma((N_CHUNKS, n_dp)), dma((N_CHUNKS, n_dp)),
            dma((n_dp * n_v,)), dma((n_dp * n_v,)),
            *codes, *codes,
        ],
        compiler_params=pltpu.CompilerParams(
            collective_id=0, has_side_effects=True, vmem_limit_bytes=60 * 1024 * 1024),
    )(hidden, weight.T, targets[None, :], pad_mask[None, :])
    return nll.reshape(t_loc), total.reshape(())


def solution(mesh):
    placed = (P("dp", "vocab"), P("dp", "vocab"), P("dp"), P("dp"))
    body = functools.partial(per_device, mesh.shape["dp"], mesh.shape["vocab"])
    return jax.shard_map(
        body, mesh=mesh, in_specs=placed, out_specs=(P("dp"), P()), check_vma=False
    )
```

```python
import functools

import jax
import jax.numpy as jnp
from jax import lax
from jax.experimental import pallas as pl
from jax.experimental.pallas import tpu as pltpu
from jax.sharding import PartitionSpec as P

N_CHUNKS = 4
LANES = 128
MESH = pl.DeviceIdType.MESH


def chunk_bounds(cols):
    width = max(LANES, cols // N_CHUNKS // LANES * LANES)
    starts = [i * width for i in range(N_CHUNKS)]
    return [(s, (cols - s) if i == N_CHUNKS - 1 else width) for i, s in enumerate(starts)]


def padded(width):
    return -(-width // LANES) * LANES


def product(tokens, heads):
    return lax.dot_general(tokens, heads, (((1,), (1,)), ((), ())), preferred_element_type=jnp.float32)


def kernel(n_dp, n_v, n_r, n_c, hid, w_hbm, tgt, msk, nll_out, tot_out,
           toks, w, acc, stat_in, stat_out, square,
           own_sem, w_sem, recv, line_send, plane_send, part_send,
           rs_send, rs_recv, st_send, st_recv, *codes):
    send_q, recv_q = codes[:N_CHUNKS], codes[N_CHUNKS:]
    t_loc, depth = hid.shape
    cols = w_hbm.shape[0]
    group = n_v // n_dp
    r_group = n_r // n_dp
    half = group // 2
    d = lax.axis_index("dp")
    v = lax.axis_index("vocab")
    k = lax.rem(v, 2)
    c = lax.rem(v // 2, n_c)
    r = v // (2 * n_c)
    way = 2 * (r // max(1, n_r // 2)) - 1

    def vid(rr, cc, kk):
        return (rr * n_c + cc) * 2 + kk

    def chunk_vid(i):
        k_off, idx = i // half, lax.rem(i, half)
        rr = d * r_group + lax.rem(idx // n_c + r, r_group)
        cc = lax.rem(idx + c, n_c)
        return vid(rr, cc, lax.rem(k + k_off, 2))

    def weight_copy(i):
        rows = pl.ds(pl.multiple_of((chunk_vid(i) - d * group) * depth, depth), depth)
        return pltpu.make_async_copy(w_hbm.at[:, rows], w.at[:, rows], w_sem.at[i])

    own = pltpu.make_async_copy(hid, toks.at[v, d], own_sem)
    own.start()

    def start_weight(i, carry):
        weight_copy(i).start()
        return carry

    lax.fori_loop(0, group, start_weight, 0)

    barrier = pltpu.get_barrier_semaphore()

    def greet(dd, vv):
        pl.semaphore_signal(barrier, inc=1, device_id={"dp": dd, "vocab": vv}, device_id_type=MESH)

    for o in range(1, n_r):
        greet(d, vid(lax.rem(r + o, n_r), c, k))
    for do in range(n_dp):
        for co in range(n_c):
            if do or co:
                greet(lax.rem(d + do, n_dp), vid(r, lax.rem(c + co, n_c), k))
    greet(d, vid(r, c, 1 - k))
    pl.semaphore_wait(barrier, n_r - 1 + n_dp * n_c - 1 + 1)

    def piece_copy(src, vv, dd, send_sem, to_d, to_v):
        return pltpu.make_async_remote_copy(
            src_ref=src, dst_ref=toks.at[vv, dd], send_sem=send_sem, recv_sem=recv.at[vv, dd],
            device_id={"dp": to_d, "vocab": to_v}, device_id_type=MESH)

    def arrived(vv, dd):
        pltpu.make_async_copy(hid, toks.at[vv, dd], recv.at[vv, dd]).wait()

    partner = vid(r, c, 1 - k)

    def line_copy(o):
        return piece_copy(hid, v, d, line_send.at[o], d, vid(lax.rem(r + n_r + way * o, n_r), c, k))

    def plane_copy(o, co):
        rr = lax.rem(r + n_r - way * o, n_r)
        mine = vid(rr, c, k)
        src = hid if o == 0 else toks.at[mine, d]
        return piece_copy(src, mine, d, plane_send.at[o, co], rr // r_group,
                          vid(r, lax.rem(c + co, n_c), k))

    def own_line_part(o):
        rr = lax.rem(r + n_r - way * o, n_r)
        mine = vid(rr, c, k)
        src = hid if o == 0 else toks.at[mine, d]
        return piece_copy(src, mine, d, part_send.at[mine // 2, d], d, partner)

    def spread(o, act):
        rr = lax.rem(r + n_r - way * o, n_r)
        home = rr // r_group == d
        for co in range(1, n_c):
            act(plane_copy(o, co))

        @pl.when(jnp.logical_not(home))
        def _():
            act(plane_copy(o, 0))

        @pl.when(home)
        def _():
            act(own_line_part(o))

    start = lambda copy: copy.start()
    sent = lambda copy: copy.wait_send()

    for o in range(1, n_r):
        line_copy(o).start()
    spread(0, start)
    for o in range(1, n_r):
        arrived(vid(lax.rem(r + n_r - way * o, n_r), c, k), d)
        spread(o, start)

    def plane_pieces(act):
        for ro in range(r_group):
            rr = d * r_group + lax.rem(r + ro, r_group)
            for do in range(n_dp):
                for co in range(n_c):
                    if do or co:
                        act(vid(rr, lax.rem(c + co, n_c), k), lax.rem(d + do, n_dp))

    def part_copy(vv, dd):
        return piece_copy(toks.at[vv, dd], vv, dd, part_send.at[vv // 2, dd], d, partner)

    def relay(vv, dd):
        arrived(vv, dd)
        part_copy(vv, dd).start()

    plane_pieces(relay)
    own.wait()

    def tokens_of(vv):
        return toks[vv].reshape(n_dp * t_loc, depth)

    def rows_of(vv):
        return pl.ds(pl.multiple_of((vv - d * group) * depth, depth), depth)

    def first_half(i, carry):
        vv = chunk_vid(i)
        weight_copy(i).wait()
        part = product(tokens_of(vv), w[:, rows_of(vv)])
        part = part.reshape(n_dp, t_loc, cols)

        @pl.when(i == 0)
        def _():
            acc[...] = part

        @pl.when(i > 0)
        def _():
            acc[...] += part

        return carry

    lax.fori_loop(0, half, first_half, 0)

    def second_ready(i, carry):
        vv = chunk_vid(i)
        weight_copy(i).wait()
        for dd in range(n_dp):
            arrived(vv, dd)
        return carry

    lax.fori_loop(half, group, second_ready, 0)

    bounds = chunk_bounds(cols)

    def rs_copy(ch, o):
        peer = lax.rem(d + o, n_dp)
        return pltpu.make_async_remote_copy(
            src_ref=send_q[ch].at[peer], dst_ref=recv_q[ch].at[d],
            send_sem=rs_send.at[ch, o], recv_sem=rs_recv.at[ch, n_dp - o],
            device_id={"dp": peer}, device_id_type=MESH)

    for ch, (lo, width) in enumerate(bounds):
        cut = slice(lo, lo + width)
        total = acc[:, :, cut].reshape(n_dp * t_loc, width)
        for i in range(half, group):
            vv = chunk_vid(i)
            total += product(tokens_of(vv), w[cut, rows_of(vv)])
        acc[:, :, cut] = total.reshape(n_dp, t_loc, width)
        for o in range(1, n_dp):
            peer = lax.rem(d + o, n_dp)
            mine = acc[peer, :, cut]
            top = jnp.maximum(jnp.max(jnp.abs(mine), axis=1, keepdims=True), 1e-30)
            expo = jnp.floor(jnp.log2(top)).astype(jnp.int32) + 2
            unit = jnp.exp2((15 - expo).astype(jnp.float32))
            code = jnp.round(mine * unit).astype(jnp.int32)
            send_q[ch][peer, :, :width] = code.astype(jnp.int16)
            wide = jnp.broadcast_to(expo, (t_loc, LANES))
            send_q[ch][peer, :, padded(width):] = wide.astype(jnp.int16)
            rs_copy(ch, o).start()

    square[...] = jnp.zeros_like(square)
    square[:, :t_loc] = jnp.broadcast_to(tgt[...].astype(jnp.float32), (LANES, t_loc))
    wanted = square[...].T[:t_loc, :1].astype(jnp.int32)
    maxes, sums, picks = [], [], []
    for ch, (lo, width) in enumerate(bounds):
        cut = slice(lo, lo + width)
        logits = acc[d, :, cut]
        for o in range(1, n_dp):
            src = lax.rem(d + n_dp - o, n_dp)
            pltpu.make_async_copy(send_q[ch].at[d], recv_q[ch].at[src], rs_recv.at[ch, n_dp - o]).wait()
            code = recv_q[ch][src, :, :width].astype(jnp.int32).astype(jnp.float32)
            expo = recv_q[ch][src, :, padded(width):].astype(jnp.int32)[:, :1]
            logits = logits + code * jnp.exp2((expo - 15).astype(jnp.float32))
        m = jnp.max(logits, axis=1, keepdims=True)
        ids = lax.broadcasted_iota(jnp.int32, (t_loc, width), 1) + (v * cols + lo)
        maxes.append(m)
        sums.append(jnp.sum(jnp.exp(logits - m), axis=1, keepdims=True))
        picks.append(jnp.sum(jnp.where(ids == wanted, logits, 0.0), axis=1, keepdims=True))
    top = functools.reduce(jnp.maximum, maxes)
    exp_sum = sum(s * jnp.exp(m - top) for s, m in zip(sums, maxes))
    pick = sum(picks)

    lane = lax.broadcasted_iota(jnp.int32, (t_loc, LANES), 1)
    packed = jnp.where(lane == 0, top, jnp.where(lane == 1, exp_sum, jnp.where(lane == 2, pick, 0.0)))
    square[...] = jnp.zeros_like(square)
    square[:t_loc, :] = packed
    stat_out[...] = square[...].T[:8, :]
    stat_out[3:4, :t_loc] = msk[...].astype(jnp.float32)
    stat_in[d, v] = stat_out[...]

    n_all = n_dp * n_v
    me = d * n_v + v

    def stat_copy(o):
        to = lax.rem(me + o, n_all)
        return pltpu.make_async_remote_copy(
            src_ref=stat_out, dst_ref=stat_in.at[d, v], send_sem=st_send.at[o],
            recv_sem=st_recv.at[n_all - o],
            device_id={"dp": to // n_v, "vocab": lax.rem(to, n_v)}, device_id_type=MESH)

    def start_stat(o, carry):
        stat_copy(o).start()
        return carry

    lax.fori_loop(1, n_all, start_stat, 0)

    def wait_stat(o, carry):
        src = lax.rem(me + o, n_all)
        pltpu.make_async_copy(
            stat_out, stat_in.at[src // n_v, lax.rem(src, n_v)], st_recv.at[o]).wait()
        return carry

    lax.fori_loop(1, n_all, wait_stat, 0)

    lane1 = lax.broadcasted_iota(jnp.int32, (1, LANES), 1)
    total = jnp.zeros((1, LANES), jnp.float32)
    for dd in range(n_dp):
        row = stat_in[dd]
        all_max = row[:, 0, :]
        m = jnp.max(all_max, axis=0, keepdims=True)
        s = jnp.sum(row[:, 1, :] * jnp.exp(all_max - m), axis=0, keepdims=True)
        p = jnp.sum(row[:, 2, :], axis=0, keepdims=True)
        nll = jnp.where(lane1 < t_loc, row[0, 3:4, :] * (m + jnp.log(s) - p), 0.0)
        total += nll

        @pl.when(d == dd)
        def _():
            nll_out[...] = nll[:, :t_loc]

    tot_out[...] = jnp.sum(total, axis=1, keepdims=True)

    for o in range(1, n_r):
        line_copy(o).wait_send()
    for o in range(n_r):
        spread(o, sent)
    plane_pieces(lambda vv, dd: part_copy(vv, dd).wait_send())
    for ch in range(N_CHUNKS):
        for o in range(1, n_dp):
            rs_copy(ch, o).wait_send()

    def end_stat(o, carry):
        stat_copy(o).wait_send()
        return carry

    lax.fori_loop(1, n_all, end_stat, 0)


def columns_of(n_chips):
    side = 1
    while side * side * 4 <= n_chips:
        side *= 2
    return side


def per_device(n_dp, n_v, hidden, weight, targets, pad_mask):
    t_loc, depth = hidden.shape
    rows, cols = weight.shape
    n_c = columns_of(n_v // 2)
    n_r = n_v // 2 // n_c
    widths = [padded(width) + LANES for _, width in chunk_bounds(cols)]
    dma = pltpu.SemaphoreType.DMA
    any_spec = pl.BlockSpec(memory_space=pl.ANY)
    vmem = pl.BlockSpec(memory_space=pltpu.VMEM)
    codes = [pltpu.VMEM((n_dp, t_loc, width), jnp.int16) for width in widths]
    nll, total = pl.pallas_call(
        functools.partial(kernel, n_dp, n_v, n_r, n_c),
        out_shape=(jax.ShapeDtypeStruct((1, t_loc), jnp.float32),
                   jax.ShapeDtypeStruct((1, 1), jnp.float32)),
        in_specs=[any_spec, any_spec, vmem, vmem],
        out_specs=(vmem, vmem),
        scratch_shapes=[
            pltpu.VMEM((n_v, n_dp, t_loc, depth), jnp.bfloat16),
            pltpu.VMEM((cols, rows), jnp.bfloat16),
            pltpu.VMEM((n_dp, t_loc, cols), jnp.float32),
            pltpu.VMEM((n_dp, n_v, 8, LANES), jnp.float32),
            pltpu.VMEM((8, LANES), jnp.float32),
            pltpu.VMEM((LANES, LANES), jnp.float32),
            dma, dma((n_v // n_dp,)), dma((n_v, n_dp)),
            dma((n_r,)), dma((n_r, n_c)), dma((n_v // 2, n_dp)),
            dma((N_CHUNKS, n_dp)), dma((N_CHUNKS, n_dp)),
            dma((n_dp * n_v,)), dma((n_dp * n_v,)),
            *codes, *codes,
        ],
        compiler_params=pltpu.CompilerParams(
            collective_id=0, has_side_effects=True, vmem_limit_bytes=60 * 1024 * 1024),
    )(hidden, weight.T, targets[None, :], pad_mask[None, :])
    return nll.reshape(t_loc), total.reshape(())


def solution(mesh):
    placed = (P("dp", "vocab"), P("dp", "vocab"), P("dp"), P("dp"))
    body = functools.partial(per_device, mesh.shape["dp"], mesh.shape["vocab"])
    return jax.shard_map(
        body, mesh=mesh, in_specs=placed, out_specs=(P("dp"), P()), check_vma=False
    )
```
